32 devices in a mesh: row: 4 (over z), col: 8 (over y, x, core).
Axes of the slice: x: 2, y: 2, z: 4, core: 2. Of those that a mesh axis runs over, the one named last changes fastest.
Arguments:
- points: float32 [64, 8192], P(None, ('row', 'col')), may hold values from -10 to 10
- start: float32 [8192], P(('row', 'col')), may hold values from -6 to 6
Outputs:
- basis: float32 [9, 8192], P(None, ('row', 'col'))
- tridiag: float32 [2, 8], replicated
The draws below stay inside these ranges and needn't reach their ends.
All inputs are finite; a program needn't handle non-finite values.
Results may differ from the reference program's by a relative error of at most 0.028.
Values may be sent and summed in bfloat16 or wider, within the bound.
A program may use at most 64 MiB of HBM per device.

```python
import jax
import jax.numpy as jnp
from jax import lax

F = 64
P_DEV = 256
ITERS = 8
NPTS = 8192


def draw_points(key, part):
    groups = max(NPTS // 128, 1)
    key_centre = jax.random.fold_in(key, 11)
    key_noise = jax.random.fold_in(key, 12)
    key_member = jax.random.fold_in(key, 13)
    member = jax.random.randint(key_member, (NPTS,), 0, groups)
    ramp = jnp.arange(NPTS).astype(jnp.float32) / max(NPTS - 1, 1)
    centres = 2.0 * jnp.clip(jax.random.normal(key_centre, (F, groups), jnp.float32), -2.5, 2.5)
    spread = 1.6 - 1.2 * ramp
    noise = jnp.clip(jax.random.normal(key_noise, (F, NPTS), jnp.float32), -3.0, 3.0) * spread[None, :]
    placed = jnp.take(centres, member, axis=1)
    return (placed + noise).astype(jnp.float32)


def levels(key, dims, split, low, largest):
    gain, own = 1.0, jax.random.fold_in(key, 6)
    for dim, blocks in split:
        heights = jnp.exp(jax.random.uniform(jax.random.fold_in(own, dim), (blocks,), jnp.float32, low / len(split), largest / len(split)))
        gain = gain * jnp.repeat(heights, dims[dim] // blocks).reshape([-1 if axis == dim else 1 for axis in range(len(dims))])
    return gain


def gaussian(key, extent, scale, most, pieces=(), held_as=jnp.bfloat16):
    gain = levels(key, extent, pieces, -0.22, 0.18) if pieces else 1.0
    array = jax.random.normal(key, extent, jnp.float32) * scale * gain
    return jnp.minimum(jnp.maximum(array, -most), most).astype(held_as)


def setup_inputs(seed: int = 0) -> dict:
    arg_keys = jax.random.split(jax.random.key(seed), 3)
    points = draw_points(jax.random.fold_in(arg_keys[2], 71), 0)
    start = gaussian(arg_keys[1], (NPTS,), 1.0, 6.0, ((0, 32),), jnp.float32)
    return dict(points=points, start=start)


def kernel_rows(row_pts, col_pts, col_sq, scale):
    cross = lax.dot_general(row_pts, col_pts, (((0,), (0,)), ((), ())), precision=lax.Precision.HIGHEST, preferred_element_type=jnp.float32)
    row_sq = lax.optimization_barrier(jnp.sum(row_pts * row_pts, axis=0))
    dist = row_sq[:, None] + col_sq[None, :] - 2.0 * cross
    return jnp.exp(-dist * scale).astype(jnp.bfloat16)

def reference(points, start):
    feats = points.shape[0]
    total = points.shape[1]
    scale = 0.5 / feats
    block = 8 * P_DEV
    col_sq = lax.optimization_barrier(jnp.sum(points * points, axis=0))
    blocks = jnp.moveaxis(points.reshape(feats, total // block, block), 1, 0)

    def apply(vec):
        vb = vec.astype(jnp.bfloat16)

        def one(pts):
            return jnp.dot(kernel_rows(pts, points, col_sq, scale), vb, preferred_element_type=jnp.float32)
        return lax.map(one, blocks).reshape(total)
    first = start / jnp.sqrt(jnp.sum(start * start) + 1e-06)
    basis = [first]
    alphas = []
    betas = []
    for step in range(ITERS):
        w = apply(basis[-1])
        stacked = jnp.stack(basis)
        h1 = jnp.dot(stacked, w, precision=lax.Precision.HIGHEST)
        w = w - jnp.dot(h1, stacked, precision=lax.Precision.HIGHEST)
        h2 = jnp.dot(stacked, w, precision=lax.Precision.HIGHEST)
        w = w - jnp.dot(h2, stacked, precision=lax.Precision.HIGHEST)
        alphas.append(h1[step])
        beta = jnp.sqrt(jnp.sum(w * w) + 1e-06)
        betas.append(beta)
        basis.append(w / beta)
    return (jnp.stack(basis), jnp.stack([jnp.stack(alphas), jnp.stack(betas)]))
```

```python
import functools
import itertools

import jax
import jax.numpy as jnp
from jax import lax
from jax.experimental import pallas as pl
from jax.experimental.pallas import tpu as pltpu
from jax.sharding import PartitionSpec as P

ITERS = 8
LANES = 128


def toggled(index, stride):
    return index + (1 - 2 * (lax.div(index, stride) % 2)) * stride


def masked(index, mask):
    for stride in mask:
        index = toggled(index, stride)
    return index


def subsets(strides):
    return [m for k in range(len(strides) + 1) for m in itertools.combinations(strides, k)]


def split(x):
    hi = x.astype(jnp.bfloat16)
    lo = (x - hi.astype(jnp.float32)).astype(jnp.bfloat16)
    return hi, lo


def body(
    R, C, points, start, basis_out, tri_out,
    gath, vecs, basis, rounded, kmat, lhs, own_sq,
    local_sem, send_sem, z_sem, half_sem, core_sem, vsend_sem, vrecv_sem,
):
    n = R * C
    feats, count = points.shape
    per = count // LANES
    rows = n * per
    half = feats // 2
    scale = 0.5 / feats
    row, col = lax.axis_index("row"), lax.axis_index("col")
    me = row * C + col

    def where(dev):
        return {"row": lax.div(dev, C), "col": lax.rem(dev, C)}

    mine = pltpu.make_async_copy(points, gath.at[me], local_sem.at[0])
    mine.start()
    first = pltpu.make_async_copy(start, vecs.at[ITERS, me], local_sem.at[1])
    first.start()

    barrier = pltpu.get_barrier_semaphore()
    for k in range(1, n):
        pl.semaphore_signal(barrier, inc=1, device_id=where(lax.rem(me + k, n)))
    basis[...] = jnp.zeros_like(basis)
    pl.semaphore_wait(barrier, n - 1)
    mine.wait()
    first.wait()

    def remote(src, dst, recv, dev, send=send_sem):
        return pltpu.make_async_remote_copy(
            src_ref=src, dst_ref=dst, send_sem=send, recv_sem=recv, device_id=where(dev)
        )

    def send_vec(slot):
        for k in range(1, n):
            dev = lax.rem(me + k, n)
            block = vecs.at[slot, me]
            remote(block, block, vrecv_sem.at[slot], dev, vsend_sem.at[slot]).start()

    def wait_vec(slot):
        some = vecs.at[slot, pl.ds(0, n - 1)]
        pltpu.make_async_copy(some, some, vrecv_sem.at[slot]).wait()

    def wait_vec_sent(slot):
        some = vecs.at[slot, pl.ds(0, n - 1)]
        pltpu.make_async_copy(some, some, vsend_sem.at[slot]).wait()

    for k in range(1, R):
        dev = lax.rem(row + k, R) * C + col
        remote(gath.at[me], gath.at[me], z_sem.at[row], dev).start()

    strides = []
    s = 2
    while s < C:
        strides.append(s)
        s *= 2
    orders = (strides, strides[::-1])

    def half_copy(order, h, stage, i, mask, r, to):
        block = gath.at[r * C + masked(col, mask), pl.ds(h * half, half)]
        return remote(block, block, half_sem.at[h, 2**stage - 1 + i, r], row * C + toggled(col, order[stage])) if to else block

    def start_stage(stage, r):
        for h, order in enumerate(orders):
            for i, mask in enumerate(subsets(order[:stage])):
                half_copy(order, h, stage, i, mask, r, True).start()

    def wait_stage(stage, r):
        for h, order in enumerate(orders):
            for i, mask in enumerate(subsets(order[:stage])):
                block = gath.at[r * C + masked(toggled(col, order[stage]), mask), pl.ds(h * half, half)]
                pltpu.make_async_copy(block, block, half_sem.at[h, 2**stage - 1 + i, r]).wait()

    combos = subsets(strides)

    def start_core(r):
        for i, mask in enumerate(combos):
            block = gath.at[r * C + masked(col, mask)]
            remote(block, block, core_sem.at[i, r], row * C + toggled(col, 1)).start()

    def wait_core(r):
        for i, mask in enumerate(combos):
            block = gath.at[r * C + masked(toggled(col, 1), mask)]
            pltpu.make_async_copy(block, block, core_sem.at[i, r]).wait()

    def group(k):
        return lax.rem(row + k, R)

    start_stage(0, row)
    send_vec(ITERS)

    own = gath[me]
    hi, lo = split(own)
    lhs[...] = jnp.concatenate([hi, hi, lo], axis=0).astype(jnp.float32).T.astype(jnp.bfloat16)
    full = hi.astype(jnp.float32) + lo.astype(jnp.float32)
    own_sq[...] = jnp.broadcast_to(jnp.sum((full * full).T, axis=1, keepdims=True), own_sq.shape)

    def make_block(dev):
        hi, lo = split(gath[dev])
        x = hi.astype(jnp.float32) + lo.astype(jnp.float32)
        sq = jnp.sum(x * x, axis=0, keepdims=True)
        rhs = jnp.concatenate([hi, lo, hi], axis=0)
        cross = jnp.dot(lhs[...], rhs, preferred_element_type=jnp.float32)
        for p in range(per):
            cut = slice(p * LANES, (p + 1) * LANES)
            dist = own_sq[...] + sq[:, cut] - 2.0 * cross[:, cut]
            kmat[dev * per + p] = jnp.exp(-dist * scale).astype(jnp.bfloat16).astype(jnp.float32)

    def make_group(r, c):
        for mask in combos:
            make_block(r * C + masked(c, mask))

    def loop(lo, hi, f):
        lax.fori_loop(lo, hi, lambda k, x: (f(k), x)[1], 0)

    def z_step(k):
        r = group(k)
        block = gath.at[r * C + col]
        pltpu.make_async_copy(block, block, z_sem.at[r]).wait()
        start_stage(0, r)

    loop(1, R, z_step)
    for stage in range(1, len(strides)):
        def mid(k, stage=stage):
            wait_stage(stage - 1, group(k))
            start_stage(stage, group(k))
        loop(0, R, mid)

    def last(k):
        wait_stage(len(strides) - 1, group(k))
        start_core(group(k))
    loop(0, R, last)
    loop(0, R, lambda k: make_group(group(k), col))

    def final(k):
        wait_core(group(k))
        make_group(group(k), toggled(col, 1))
    loop(0, R, final)

    pltpu.make_async_copy(gath.at[pl.ds(0, n - 1)], gath.at[pl.ds(0, n - 1)], send_sem).wait()

    def total(x):
        return jnp.sum(x, keepdims=True)

    wait_vec(ITERS)
    wait_vec_sent(ITERS)
    s = vecs[ITERS].reshape(rows, LANES)

    def keep(j, q):
        basis[j] = q
        rounded[...] = q.astype(jnp.bfloat16).astype(jnp.float32)

    keep(0, s / jnp.sqrt(total(s * s) + 1e-06))

    lane = lax.broadcasted_iota(jnp.int32, (2, LANES), 1)
    sub = lax.broadcasted_iota(jnp.int32, (2, LANES), 0)

    def step(j, tri):
        def chunk(c, acc):
            return acc + kmat[c] * rounded[pl.ds(c, 1), :]

        acc = lax.fori_loop(0, rows, chunk, jnp.zeros((count, LANES), jnp.float32), unroll=4)
        mine = jnp.sum(acc.T, axis=0, keepdims=True)
        for p in range(per):
            vecs[j, me, p : p + 1, :] = mine[:, p * LANES : (p + 1) * LANES]
        send_vec(j)
        wait_vec(j)
        wait_vec_sent(j)
        w = vecs[j].reshape(rows, LANES)
        h1 = [total(basis[i] * w) for i in range(ITERS)]
        for i in range(ITERS):
            w = w - h1[i] * basis[i]
        h2 = [total(basis[i] * w) for i in range(ITERS)]
        for i in range(ITERS):
            w = w - h2[i] * basis[i]
        beta = jnp.sqrt(total(w * w) + 1e-06)
        keep(j + 1, w / beta)
        alpha = sum(jnp.where(j == i, h, 0.0) for i, h in enumerate(h1))
        return jnp.where(lane == j, jnp.where(sub == 0, alpha, beta), tri)

    tri = lax.fori_loop(0, ITERS, step, jnp.zeros((2, LANES), jnp.float32))
    tri_out[...] = tri[:, :ITERS]
    basis_out[...] = basis[:, pl.ds(me * per, per), :]


def per_device(R, C, points, start):
    feats, count = points.shape
    n = R * C
    per = count // LANES
    rows = n * per
    vmem = pl.BlockSpec(memory_space=pltpu.VMEM)
    anywhere = pl.BlockSpec(memory_space=pl.ANY)
    basis, tri = pl.pallas_call(
        functools.partial(body, R, C),
        out_shape=(
            jax.ShapeDtypeStruct((ITERS + 1, per, LANES), jnp.float32),
            jax.ShapeDtypeStruct((2, ITERS), jnp.float32),
        ),
        in_specs=[anywhere, anywhere],
        out_specs=(vmem, vmem),
        scratch_shapes=[
            pltpu.VMEM((n, feats, count), jnp.float32),
            pltpu.VMEM((ITERS + 1, n, per, LANES), jnp.float32),
            pltpu.VMEM((ITERS + 1, rows, LANES), jnp.float32),
            pltpu.VMEM((rows, LANES), jnp.float32),
            pltpu.VMEM((rows, count, LANES), jnp.float32),
            pltpu.VMEM((count, 3 * feats), jnp.bfloat16),
            pltpu.VMEM((count, LANES), jnp.float32),
            pltpu.SemaphoreType.DMA((2,)),
            pltpu.SemaphoreType.DMA,
            pltpu.SemaphoreType.DMA((R,)),
            pltpu.SemaphoreType.DMA((2, C // 2 - 1, R)),
            pltpu.SemaphoreType.DMA((C // 2, R)),
            pltpu.SemaphoreType.DMA((ITERS + 1,)),
            pltpu.SemaphoreType.DMA((ITERS + 1,)),
        ],
        compiler_params=pltpu.CompilerParams(
            collective_id=0, has_side_effects=True, vmem_limit_bytes=60 * 1024 * 1024
        ),
    )(points, start.reshape(per, LANES))
    return basis.reshape(ITERS + 1, count), tri


def solution(mesh):
    R, C = mesh.shape["row"], mesh.shape["col"]
    return jax.shard_map(
        functools.partial(per_device, R, C),
        mesh=mesh,
        in_specs=(P(None, ("row", "col")), P(("row", "col"))),
        out_specs=(P(None, ("row", "col")), P()),
        check_vma=False,
    )
```

```python
import functools
import itertools

import jax
import jax.numpy as jnp
from jax import lax
from jax.experimental import pallas as pl
from jax.experimental.pallas import tpu as pltpu
from jax.sharding import PartitionSpec as P

ITERS = 8
LANES = 128


def toggled(index, stride):
    return index + (1 - 2 * (lax.div(index, stride) % 2)) * stride


def masked(index, mask):
    for stride in mask:
        index = toggled(index, stride)
    return index


def subsets(strides):
    return [m for k in range(len(strides) + 1) for m in itertools.combinations(strides, k)]


def split(x):
    hi = x.astype(jnp.bfloat16)
    lo = (x - hi.astype(jnp.float32)).astype(jnp.bfloat16)
    return hi, lo


def body(
    R, C, points, start, out,
    gath, vecs, basis, rounded, kmat, lhs, own_sq,
    local_sem, send_sem, z_sem, half_sem, core_sem, vsend_sem, vrecv_sem,
):
    n = R * C
    feats, count = points.shape
    per = count // LANES
    rows = n * per
    half = feats // 2
    scale = 0.5 / feats
    row, col = lax.axis_index("row"), lax.axis_index("col")
    me = row * C + col

    def where(dev):
        return {"row": lax.div(dev, C), "col": lax.rem(dev, C)}

    mine = pltpu.make_async_copy(points, gath.at[me], local_sem.at[0])
    mine.start()
    first = pltpu.make_async_copy(start, vecs.at[ITERS, pl.ds(pl.multiple_of(me * per, per), per)], local_sem.at[1])
    first.start()

    barrier = pltpu.get_barrier_semaphore()
    for k in range(1, n):
        pl.semaphore_signal(barrier, inc=1, device_id=where(lax.rem(me + k, n)))
    basis[...] = jnp.zeros_like(basis)
    pl.semaphore_wait(barrier, n - 1)
    mine.wait()
    first.wait()

    def remote(src, dst, recv, dev, send=send_sem):
        return pltpu.make_async_remote_copy(
            src_ref=src, dst_ref=dst, send_sem=send, recv_sem=recv, device_id=where(dev)
        )

    def send_vec(slot):
        for k in range(1, n):
            dev = lax.rem(me + k, n)
            block = vecs.at[slot, pl.ds(pl.multiple_of(me * per, per), per)]
            remote(block, block, vrecv_sem.at[slot], dev, vsend_sem.at[slot]).start()

    def wait_vec(slot):
        some = vecs.at[slot, pl.ds(0, rows - per)]
        pltpu.make_async_copy(some, some, vrecv_sem.at[slot]).wait()

    def wait_vec_sent(slot):
        some = vecs.at[slot, pl.ds(0, rows - per)]
        pltpu.make_async_copy(some, some, vsend_sem.at[slot]).wait()

    def group(k):
        return masked(row, [1 << t for t in range(k.bit_length()) if k >> t & 1])

    for k in range(1, R):
        dev = group(k) * C + col
        remote(gath.at[me], gath.at[me], z_sem.at[row], dev).start()

    strides = []
    s = 2
    while s < C:
        strides.append(s)
        s *= 2
    orders = (strides, strides[::-1])

    def half_copy(order, h, stage, i, mask, r, to):
        block = gath.at[r * C + masked(col, mask), pl.ds(h * half, half)]
        return remote(block, block, half_sem.at[h, 2**stage - 1 + i, r], row * C + toggled(col, order[stage])) if to else block

    def start_stage(stage, r):
        for h, order in enumerate(orders):
            for i, mask in enumerate(subsets(order[:stage])):
                half_copy(order, h, stage, i, mask, r, True).start()

    def wait_stage(stage, r):
        for h, order in enumerate(orders):
            for i, mask in enumerate(subsets(order[:stage])):
                block = gath.at[r * C + masked(toggled(col, order[stage]), mask), pl.ds(h * half, half)]
                pltpu.make_async_copy(block, block, half_sem.at[h, 2**stage - 1 + i, r]).wait()

    combos = subsets(strides)

    def start_core(r):
        for i, mask in enumerate(combos):
            block = gath.at[r * C + masked(col, mask)]
            remote(block, block, core_sem.at[i, r], row * C + toggled(col, 1)).start()

    def wait_core(r):
        for i, mask in enumerate(combos):
            block = gath.at[r * C + masked(toggled(col, 1), mask)]
            pltpu.make_async_copy(block, block, core_sem.at[i, r]).wait()

    start_stage(0, row)
    send_vec(ITERS)

    own = gath[me]
    hi, lo = split(own)
    lhs[...] = jnp.concatenate([hi, hi, lo], axis=0).astype(jnp.float32).T.astype(jnp.bfloat16)
    full = hi.astype(jnp.float32) + lo.astype(jnp.float32)
    own_sq[...] = jnp.broadcast_to(jnp.sum((full * full).T, axis=1, keepdims=True), own_sq.shape)

    def make_block(dev):
        hi, lo = split(gath[dev])
        x = hi.astype(jnp.float32) + lo.astype(jnp.float32)
        sq = jnp.sum(x * x, axis=0, keepdims=True)
        rhs = jnp.concatenate([hi, lo, hi], axis=0)
        cross = jnp.dot(lhs[...], rhs, preferred_element_type=jnp.float32)
        for p in range(per):
            cut = slice(p * LANES, (p + 1) * LANES)
            dist = own_sq[...] + sq[:, cut] - 2.0 * cross[:, cut]
            kmat[dev * per + p] = jnp.exp(-dist * scale).astype(jnp.bfloat16).astype(jnp.float32)

    def make_group(r, c):
        for mask in combos:
            make_block(r * C + masked(c, mask))

    depth = len(strides)
    for t in range(R + depth + 1):
        if 0 < t < R:
            block = gath.at[group(t) * C + col]
            pltpu.make_async_copy(block, block, z_sem.at[group(t)]).wait()
            start_stage(0, group(t))
        for stage in range(1, depth):
            if 0 <= t - stage < R:
                wait_stage(stage - 1, group(t - stage))
                start_stage(stage, group(t - stage))
        if 0 <= t - depth < R:
            wait_stage(depth - 1, group(t - depth))
            start_core(group(t - depth))
            make_group(group(t - depth), col)
        if 0 <= t - depth - 1 < R:
            wait_core(group(t - depth - 1))
            make_group(group(t - depth - 1), toggled(col, 1))

    pltpu.make_async_copy(gath.at[pl.ds(0, n - 1)], gath.at[pl.ds(0, n - 1)], send_sem).wait()

    def dots(w):
        parts = [jnp.sum((basis[i] * w).reshape(rows // 8, 8, LANES), axis=0) for i in range(ITERS)]
        cols = jnp.sum(jnp.concatenate([jnp.sum(x, axis=0, keepdims=True) for x in parts], axis=0), axis=1, keepdims=True)
        return [cols[i : i + 1] for i in range(ITERS)]

    def total(x):
        return jnp.sum(x, keepdims=True)

    wait_vec(ITERS)
    wait_vec_sent(ITERS)
    s = vecs[ITERS]

    def keep(j, q):
        basis[j] = q
        rounded[...] = q.astype(jnp.bfloat16).astype(jnp.float32)

    keep(0, s / jnp.sqrt(total(s * s) + 1e-06))

    lane = lax.broadcasted_iota(jnp.int32, (2, LANES), 1)
    sub = lax.broadcasted_iota(jnp.int32, (2, LANES), 0)

    def step(j, tri):
        def chunk(c, acc):
            return acc + kmat[c] * rounded[pl.ds(c, 1), :]

        acc = lax.fori_loop(0, rows, chunk, jnp.zeros((count, LANES), jnp.float32), unroll=16)
        mine = jnp.sum(acc.T, axis=0, keepdims=True)
        for p in range(per):
            vecs[j, pl.ds(me * per + p, 1), :] = mine[:, p * LANES : (p + 1) * LANES]
        send_vec(j)
        wait_vec(j)
        wait_vec_sent(j)
        w = vecs[j]
        h1 = dots(w)
        for i in range(ITERS):
            w = w - h1[i] * basis[i]
        h2 = dots(w)
        for i in range(ITERS):
            w = w - h2[i] * basis[i]
        beta = jnp.sqrt(total(w * w) + 1e-06)
        keep(j + 1, w / beta)
        alpha = sum(jnp.where(j == i, h, 0.0) for i, h in enumerate(h1))
        return jnp.where(lane == j, jnp.where(sub == 0, alpha, beta), tri)

    tri = lax.fori_loop(0, ITERS, step, jnp.zeros((2, LANES), jnp.float32))
    for p in range(per):
        cut = slice(p * LANES, (p + 1) * LANES)
        for j in range(ITERS + 1):
            out[j : j + 1, cut] = basis[j, pl.ds(me * per + p, 1), :]
    out[ITERS + 1 : ITERS + 3, :LANES] = tri


def per_device(R, C, points, start):
    feats, count = points.shape
    n = R * C
    per = count // LANES
    rows = n * per
    vmem = pl.BlockSpec(memory_space=pltpu.VMEM)
    anywhere = pl.BlockSpec(memory_space=pl.ANY)
    out = pl.pallas_call(
        functools.partial(body, R, C),
        out_shape=jax.ShapeDtypeStruct((ITERS + 3, count), jnp.float32),
        in_specs=[anywhere, anywhere],
        out_specs=vmem,
        scratch_shapes=[
            pltpu.VMEM((n, feats, count), jnp.float32),
            pltpu.VMEM((ITERS + 1, rows, LANES), jnp.float32),
            pltpu.VMEM((ITERS + 1, rows, LANES), jnp.float32),
            pltpu.VMEM((rows, LANES), jnp.float32),
            pltpu.VMEM((rows, count, LANES), jnp.float32),
            pltpu.VMEM((count, 3 * feats), jnp.bfloat16),
            pltpu.VMEM((count, LANES), jnp.float32),
            pltpu.SemaphoreType.DMA((2,)),
            pltpu.SemaphoreType.DMA,
            pltpu.SemaphoreType.DMA((R,)),
            pltpu.SemaphoreType.DMA((2, C // 2 - 1, R)),
            pltpu.SemaphoreType.DMA((C // 2, R)),
            pltpu.SemaphoreType.DMA((ITERS + 1,)),
            pltpu.SemaphoreType.DMA((ITERS + 1,)),
        ],
        compiler_params=pltpu.CompilerParams(
            collective_id=0, has_side_effects=True, vmem_limit_bytes=60 * 1024 * 1024
        ),
    )(points, start.reshape(per, LANES))
    return out[: ITERS + 1], out[ITERS + 1 :, :ITERS]


def solution(mesh):
    R, C = mesh.shape["row"], mesh.shape["col"]
    return jax.shard_map(
        functools.partial(per_device, R, C),
        mesh=mesh,
        in_specs=(P(None, ("row", "col")), P(("row", "col"))),
        out_specs=(P(None, ("row", "col")), P()),
        check_vma=False,
    )
```

```python
import functools
import itertools

import jax
import jax.numpy as jnp
from jax import lax
from jax.experimental import pallas as pl
from jax.experimental.pallas import tpu as pltpu
from jax.sharding import PartitionSpec as P

ITERS = 8
LANES = 128


def toggled(index, stride):
    return index + (1 - 2 * (lax.div(index, stride) % 2)) * stride


def masked(index, mask):
    for stride in mask:
        index = toggled(index, stride)
    return index


def subsets(strides):
    return [m for k in range(len(strides) + 1) for m in itertools.combinations(strides, k)]


def split(x):
    hi = x.astype(jnp.bfloat16)
    lo = (x - hi.astype(jnp.float32)).astype(jnp.bfloat16)
    return hi, lo


def body(
    R, C, points, start, out,
    gath, vecs, basis, rounded, kmat, lhs, own_sq,
    local_sem, send_sem, z_sem, half_sem, core_sem, vsend_sem, vrecv_sem,
):
    n = R * C
    feats, count = points.shape
    per = count // LANES
    rows = n * per
    half = feats // 2
    scale = 0.5 / feats
    row, col = lax.axis_index("row"), lax.axis_index("col")
    me = row * C + col

    def where(dev):
        return {"row": lax.div(dev, C), "col": lax.rem(dev, C)}

    mine = pltpu.make_async_copy(points, gath.at[me], local_sem.at[0])
    mine.start()
    first = pltpu.make_async_copy(start, vecs.at[ITERS, pl.ds(pl.multiple_of(me * per, per), per)], local_sem.at[1])
    first.start()

    barrier = pltpu.get_barrier_semaphore()
    for k in range(1, n):
        pl.semaphore_signal(barrier, inc=1, device_id=where(lax.rem(me + k, n)))
    basis[...] = jnp.zeros_like(basis)
    pl.semaphore_wait(barrier, n - 1)
    mine.wait()
    first.wait()

    def remote(src, dst, recv, dev, send=send_sem):
        return pltpu.make_async_remote_copy(
            src_ref=src, dst_ref=dst, send_sem=send, recv_sem=recv, device_id=where(dev)
        )

    def xor(index, mask):
        return masked(index, [1 << t for t in range(mask.bit_length()) if mask >> t & 1])

    row_of = [xor(row, k) for k in range(R)]
    col_of = [xor(col, k) for k in range(C)]
    far_first = sorted(range(1, n), key=lambda k: (-(k // C), -(k % C).bit_count()))

    def send_vec(slot):
        block = vecs.at[slot, pl.ds(pl.multiple_of(me * per, per), per)]
        for k in far_first:
            pltpu.make_async_remote_copy(
                src_ref=block,
                dst_ref=block,
                send_sem=vsend_sem.at[slot],
                recv_sem=vrecv_sem.at[slot],
                device_id={"row": row_of[k // C], "col": col_of[k % C]},
            ).start()

    def wait_vec(slot):
        some = vecs.at[slot, pl.ds(0, rows - per)]
        pltpu.make_async_copy(some, some, vrecv_sem.at[slot]).wait()

    def wait_vec_sent(slot):
        some = vecs.at[slot, pl.ds(0, rows - per)]
        pltpu.make_async_copy(some, some, vsend_sem.at[slot]).wait()

    def group(k):
        return masked(row, [1 << t for t in range(k.bit_length()) if k >> t & 1])

    for k in range(1, R):
        dev = group(k) * C + col
        remote(gath.at[me], gath.at[me], z_sem.at[row], dev).start()

    strides = []
    s = 2
    while s < C:
        strides.append(s)
        s *= 2
    orders = (strides, strides[::-1])

    def half_copy(order, h, stage, i, mask, r, to):
        block = gath.at[r * C + masked(col, mask), pl.ds(h * half, half)]
        return remote(block, block, half_sem.at[h, 2**stage - 1 + i, r], row * C + toggled(col, order[stage])) if to else block

    def start_stage(stage, r):
        for h, order in enumerate(orders):
            for i, mask in enumerate(subsets(order[:stage])):
                half_copy(order, h, stage, i, mask, r, True).start()

    def wait_stage(stage, r):
        for h, order in enumerate(orders):
            for i, mask in enumerate(subsets(order[:stage])):
                block = gath.at[r * C + masked(toggled(col, order[stage]), mask), pl.ds(h * half, half)]
                pltpu.make_async_copy(block, block, half_sem.at[h, 2**stage - 1 + i, r]).wait()

    combos = subsets(strides)

    def start_core(r):
        for i, mask in enumerate(combos):
            block = gath.at[r * C + masked(col, mask)]
            remote(block, block, core_sem.at[i, r], row * C + toggled(col, 1)).start()

    def wait_core(r):
        for i, mask in enumerate(combos):
            block = gath.at[r * C + masked(toggled(col, 1), mask)]
            pltpu.make_async_copy(block, block, core_sem.at[i, r]).wait()

    start_stage(0, row)
    send_vec(ITERS)

    own = gath[me]
    hi, lo = split(own)
    lhs[...] = jnp.concatenate([hi, hi, lo], axis=0).astype(jnp.float32).T.astype(jnp.bfloat16)
    full = hi.astype(jnp.float32) + lo.astype(jnp.float32)
    own_sq[...] = jnp.broadcast_to(jnp.sum((full * full).T, axis=1, keepdims=True), own_sq.shape)

    def make_block(dev):
        hi, lo = split(gath[dev])
        x = hi.astype(jnp.float32) + lo.astype(jnp.float32)
        sq = jnp.sum(x * x, axis=0, keepdims=True)
        rhs = jnp.concatenate([hi, lo, hi], axis=0)
        cross = jnp.dot(lhs[...], rhs, preferred_element_type=jnp.float32)
        for p in range(per):
            cut = slice(p * LANES, (p + 1) * LANES)
            dist = own_sq[...] + sq[:, cut] - 2.0 * cross[:, cut]
            kmat[dev * per + p] = jnp.exp(-dist * scale).astype(jnp.bfloat16).astype(jnp.float32)

    def make_group(r, c):
        for mask in combos:
            make_block(r * C + masked(c, mask))

    depth = len(strides)
    for t in range(R + depth + 1):
        if 0 < t < R:
            block = gath.at[group(t) * C + col]
            pltpu.make_async_copy(block, block, z_sem.at[group(t)]).wait()
            start_stage(0, group(t))
        for stage in range(1, depth):
            if 0 <= t - stage < R:
                wait_stage(stage - 1, group(t - stage))
                start_stage(stage, group(t - stage))
        if 0 <= t - depth < R:
            wait_stage(depth - 1, group(t - depth))
            start_core(group(t - depth))
            make_group(group(t - depth), col)
        if 0 <= t - depth - 1 < R:
            wait_core(group(t - depth - 1))
            make_group(group(t - depth - 1), toggled(col, 1))

    pltpu.make_async_copy(gath.at[pl.ds(0, n - 1)], gath.at[pl.ds(0, n - 1)], send_sem).wait()

    def dots(w):
        parts = [jnp.sum((basis[i] * w).reshape(rows // 8, 8, LANES), axis=0) for i in range(ITERS)]
        cols = jnp.sum(jnp.concatenate([jnp.sum(x, axis=0, keepdims=True) for x in parts], axis=0), axis=1, keepdims=True)
        return [cols[i : i + 1] for i in range(ITERS)]

    def total(x):
        return jnp.sum(x, keepdims=True)

    wait_vec(ITERS)
    s = vecs[ITERS]

    def keep(j, q):
        basis[j] = q
        rounded[...] = q.astype(jnp.bfloat16).astype(jnp.float32)

    keep(0, s / jnp.sqrt(total(s * s) + 1e-06))

    lane = lax.broadcasted_iota(jnp.int32, (2, LANES), 1)
    sub = lax.broadcasted_iota(jnp.int32, (2, LANES), 0)

    def step(j, tri):
        def chunk(c, acc):
            return acc + kmat[c] * rounded[pl.ds(c, 1), :]

        for p in range(per):
            def chunk(c, acc, p=p):
                return acc + kmat[c, p * LANES : (p + 1) * LANES] * rounded[pl.ds(c, 1), :]

            acc = lax.fori_loop(0, rows, chunk, jnp.zeros((LANES, LANES), jnp.float32), unroll=32)
            vecs[j, pl.ds(me * per + p, 1), :] = jnp.sum(acc.T, axis=0, keepdims=True)
        send_vec(j)
        wait_vec(j)
        w = vecs[j]
        h1 = dots(w)
        for i in range(ITERS):
            w = w - h1[i] * basis[i]
        h2 = dots(w)
        for i in range(ITERS):
            w = w - h2[i] * basis[i]
        beta = jnp.sqrt(total(w * w) + 1e-06)
        keep(j + 1, w / beta)
        alpha = sum(jnp.where(j == i, h, 0.0) for i, h in enumerate(h1))
        return jnp.where(lane == j, jnp.where(sub == 0, alpha, beta), tri)

    tri = lax.fori_loop(0, ITERS, step, jnp.zeros((2, LANES), jnp.float32))
    for p in range(per):
        cut = slice(p * LANES, (p + 1) * LANES)
        for j in range(ITERS + 1):
            out[j : j + 1, cut] = basis[j, pl.ds(me * per + p, 1), :]
    out[ITERS + 1 : ITERS + 3, :LANES] = tri
    lax.fori_loop(0, ITERS + 1, lambda j, x: (wait_vec_sent(j), x)[1], 0)


def per_device(R, C, points, start):
    feats, count = points.shape
    n = R * C
    per = count // LANES
    rows = n * per
    vmem = pl.BlockSpec(memory_space=pltpu.VMEM)
    anywhere = pl.BlockSpec(memory_space=pl.ANY)
    out = pl.pallas_call(
        functools.partial(body, R, C),
        out_shape=jax.ShapeDtypeStruct((ITERS + 3, count), jnp.float32),
        in_specs=[anywhere, anywhere],
        out_specs=vmem,
        scratch_shapes=[
            pltpu.VMEM((n, feats, count), jnp.float32),
            pltpu.VMEM((ITERS + 1, rows, LANES), jnp.float32),
            pltpu.VMEM((ITERS + 1, rows, LANES), jnp.float32),
            pltpu.VMEM((rows, LANES), jnp.float32),
            pltpu.VMEM((rows, count, LANES), jnp.float32),
            pltpu.VMEM((count, 3 * feats), jnp.bfloat16),
            pltpu.VMEM((count, LANES), jnp.float32),
            pltpu.SemaphoreType.DMA((2,)),
            pltpu.SemaphoreType.DMA,
            pltpu.SemaphoreType.DMA((R,)),
            pltpu.SemaphoreType.DMA((2, C // 2 - 1, R)),
            pltpu.SemaphoreType.DMA((C // 2, R)),
            pltpu.SemaphoreType.DMA((ITERS + 1,)),
            pltpu.SemaphoreType.DMA((ITERS + 1,)),
        ],
        compiler_params=pltpu.CompilerParams(
            collective_id=0, has_side_effects=True, vmem_limit_bytes=60 * 1024 * 1024
        ),
    )(points, start.reshape(per, LANES))
    return out[: ITERS + 1], out[ITERS + 1 :, :ITERS]


def solution(mesh):
    R, C = mesh.shape["row"], mesh.shape["col"]
    return jax.shard_map(
        functools.partial(per_device, R, C),
        mesh=mesh,
        in_specs=(P(None, ("row", "col")), P(("row", "col"))),
        out_specs=(P(None, ("row", "col")), P()),
        check_vma=False,
    )
```
